32 devices in a mesh: dp: 2 (over y), expert: 16 (over z, x, core).
Axes of the slice: x: 2, y: 2, z: 4, core: 2. Of those that a mesh axis runs over, the one named last changes fastest.
Arguments:
- routed: bfloat16 [4096, 7168], P(('dp', 'expert')), may hold values from -160 to 160
- expert_ids: int32 [4096, 8], P(('dp', 'expert')), may hold values from 0 to 127, all different within a row
- norm_gain: bfloat16 [7168], replicated, may hold values from 0.099609375 to 1.8984375
- gate_weight: bfloat16 [16, 7168, 2048], P('expert', None, 'dp'), may hold values from -0.0625 to 0.0625
- up_weight: bfloat16 [16, 7168, 2048], P('expert', None, 'dp'), may hold values from -0.0625 to 0.0625
- down_weight: bfloat16 [16, 2048, 7168], P('expert', 'dp'), may hold values from -0.125 to 0.125
- old_place: int32 [16], replicated, may hold values from 0 to 127, as said below
- new_place: int32 [16], replicated, may hold values from 0 to 127, as said below
- probe_ids: int32 [1280], P(('dp', 'expert')), may hold values from 0 to 127
Outputs:
- expert_load: float32 [128], P('expert')
- expert_energy: float32 [128], P('expert')
- probe_out: bfloat16 [1280, 7168], P(('dp', 'expert'))
The draws below stay inside these ranges and needn't reach their ends.
Inputs may be any that keep to these rules, and one draw needn't show every extreme that they name: `old_place`: 16 different experts. `new_place`: the same 16 experts as old_place, in some order.
All inputs are finite; a program needn't handle non-finite values.
Results may differ from the reference program's by a relative error of at most 0.012.
Values may be sent and summed in bfloat16 or wider, within the bound.
A program may use at most 128 MiB of HBM per device.

```python
import jax
import jax.numpy as jnp
from jax import lax

D = 7168
FF = 2048
TOP = 8
TOK_DEV = 128
PROBE = 40
EXPERTS = 128
SLOTS = 16
TOKENS = 4096
PROBES = 1280
N_DP = 2


def draw_routed(key, part):
    first = jax.random.fold_in(key, 101)
    second = jax.random.fold_in(key, 202)
    third = jax.random.fold_in(key, 303)
    row_scale = jnp.exp(jax.random.uniform(second, (TOKENS, 1), minval=-1.15, maxval=1.15))
    column_scale = jnp.exp(jax.random.uniform(third, (1, D), minval=-1.15, maxval=1.15))
    rising = jnp.exp(jnp.log(3.0) * (jnp.arange(TOKENS, dtype=jnp.float32) / TOKENS - 0.5))[:, None]
    values = jnp.clip(jax.random.normal(first, (TOKENS, D)), -4.0, 4.0)
    return (values * row_scale * column_scale * rising).astype(jnp.bfloat16)


def draw_plan(key):
    base = jax.random.fold_in(key, 17)
    chosen = jax.random.permutation(jax.random.fold_in(base, 1), EXPERTS)[:SLOTS]
    order = jax.random.permutation(jax.random.fold_in(base, 2), SLOTS)
    return (chosen.astype(jnp.int32), jnp.take(chosen, order).astype(jnp.int32))


def draw_old_place(key, part):
    return draw_plan(key)[0]


def draw_new_place(key, part):
    return draw_plan(key)[1]


def with_ends(values, own_key, least, high):
    longest = values.shape.index(max(values.shape))
    spots = []
    for shift in (0, 1):
        where = [jax.random.randint(jax.random.fold_in(own_key, axis), (), 0, length) for axis, length in enumerate(values.shape)]
        where[longest] = (where[longest] + shift) % values.shape[longest]
        spots.append(tuple(where))
    return values.at[spots[0]].set(least).at[spots[1]].set(high)


def block_levels(stream_key, extent, pieces, low, top_value):
    level, own = 1.0, jax.random.fold_in(stream_key, 6)
    for dim, parts in pieces:
        steps = jnp.exp(jax.random.uniform(jax.random.fold_in(own, dim), (parts,), jnp.float32, low / len(pieces), top_value / len(pieces)))
        level = level * jnp.repeat(steps, extent[dim] // parts).reshape([-1 if axis == dim else 1 for axis in range(len(extent))])
    return level


def picks_of(rng, rows, count, top, lift):
    ranking = jax.random.permutation(jax.random.fold_in(rng, 1), count)
    pull = ranking
    for power in range(3):
        pull = pull * pull // count
    pull = pull * lift // count
    tickets = jax.random.randint(jax.random.fold_in(rng, 2), (rows, count), 0, 4096) + pull
    holders = jax.random.permutation(jax.random.fold_in(rng, 3), rows)[jnp.arange(count) % rows]
    tickets = jnp.where(jnp.arange(rows)[:, None] == holders[None, :], 1 << 14, tickets)
    merit = tickets * count + jnp.arange(count)
    return lax.top_k(merit.astype(jnp.int32), top)[1].astype(jnp.int32)


def noise(stream_key, shape, deviation, most, cuts=(), kind=jnp.bfloat16):
    array = deviation * jax.random.normal(stream_key, shape, jnp.float32)
    if cuts:
        array = array * block_levels(stream_key, shape, cuts, -0.22, 0.18)
    return jnp.clip(array, -most, most).astype(kind)


def setup_inputs(seed: int = 0) -> dict:
    seeds = jax.random.split(jax.random.key(seed), 10)
    return {
        "routed": draw_routed(jax.random.fold_in(seeds[9], 71), 0),
        "expert_ids": picks_of(seeds[1], TOKENS, EXPERTS, TOP, 1024),
        "norm_gain": jnp.clip(1.0 + 0.18 * jax.random.normal(seeds[2], (D,), jnp.float32), 0.099609375, 1.8984375).astype(jnp.bfloat16),
        "gate_weight": noise(seeds[3], (SLOTS, D, FF), D ** -0.5, 0.0625, ((0, 16), (2, 2))),
        "up_weight": noise(seeds[4], (SLOTS, D, FF), D ** -0.5, 0.0625, ((0, 16), (2, 2))),
        "down_weight": noise(seeds[5], (SLOTS, FF, D), FF ** -0.5, 0.125, ((0, 16), (1, 2))),
        "old_place": draw_old_place(jax.random.fold_in(seeds[9], 71), 0),
        "new_place": draw_new_place(jax.random.fold_in(seeds[9], 71), 0),
        "probe_ids": with_ends(jax.random.randint(seeds[8], (PROBES,), 0, TOK_DEV), jax.random.fold_in(seeds[8], 1), 0, TOK_DEV - 1).astype(jnp.int32),
    }


epsilon = 1e-06

def block_stats(block):
    token_rows, id_block = block
    features = token_rows.astype(jnp.float32)
    mean_square = lax.optimization_barrier(jnp.sum(features * features, axis=1)) / D
    positions = jnp.arange(EXPERTS, dtype=jnp.int32)
    onehot = lax.optimization_barrier(jnp.sum((id_block[:, :, None] == positions[None, None, :]).astype(jnp.float32), axis=1))
    columns = jnp.stack([jnp.ones_like(mean_square), mean_square])
    return (jnp.dot(columns, onehot, precision=lax.Precision.HIGHEST), mean_square)

def reference(routed, expert_ids, norm_gain, gate_weight, up_weight, down_weight, old_place, new_place, probe_ids):
    blocks = TOKENS // TOK_DEV
    stats, mean_square = lax.map(block_stats, (routed.reshape(blocks, TOK_DEV, D), expert_ids.reshape(blocks, TOK_DEV, TOP)))
    totals = lax.optimization_barrier(jnp.sum(stats, axis=0))
    counts = totals[0]
    expert_load = counts * EXPERTS / (TOKENS * TOP)
    expert_energy = totals[1] / counts
    mean_square = mean_square.reshape(TOKENS)
    offsets = jnp.arange(PROBES, dtype=jnp.int32) // PROBE * TOK_DEV
    picked = (offsets + probe_ids).astype(jnp.int32)
    picked_rows = jnp.take(routed, picked, axis=0).astype(jnp.float32)
    scale = lax.rsqrt(jnp.take(mean_square, picked) + epsilon)
    normed = (picked_rows * scale[:, None] * norm_gain.astype(jnp.float32)[None, :]).astype(jnp.bfloat16)
    grouped = normed.reshape(N_DP, SLOTS, PROBE, D)
    slot_index = jnp.arange(SLOTS, dtype=jnp.int32)
    hidden_block = FF // N_DP

    def per_slot(slot_number):
        holder = jnp.sum(jnp.where(old_place == new_place[slot_number], slot_index, 0)).astype(jnp.int32)
        inputs = lax.dynamic_index_in_dim(grouped, slot_number, 1, keepdims=False).reshape(N_DP * PROBE, D)
        gate_matrix = lax.dynamic_index_in_dim(gate_weight, holder, 0, keepdims=False)
        up_matrix = lax.dynamic_index_in_dim(up_weight, holder, 0, keepdims=False)
        down_matrix = lax.dynamic_index_in_dim(down_weight, holder, 0, keepdims=False)
        gate_value = jnp.dot(inputs, gate_matrix, preferred_element_type=jnp.float32)
        up_value = jnp.dot(inputs, up_matrix, preferred_element_type=jnp.float32)
        hidden = (jax.nn.silu(gate_value) * up_value).astype(jnp.bfloat16)
        running = jnp.zeros((N_DP * PROBE, D), jnp.float32)
        for group_index in range(N_DP):
            lower = group_index * hidden_block
            partial_value = jnp.dot(hidden[:, lower:lower + hidden_block], down_matrix[lower:lower + hidden_block], preferred_element_type=jnp.float32).astype(jnp.bfloat16)
            partial_value = lax.optimization_barrier(partial_value)
            running = running + partial_value.astype(jnp.float32)
        return running.astype(jnp.bfloat16).reshape(N_DP, PROBE, D)
    results = lax.map(per_slot, slot_index)
    probe_out = jnp.transpose(results, (1, 0, 2, 3)).reshape(PROBES, D)
    return (expert_load, expert_energy, probe_out)
```

```python
import functools

import jax
import jax.numpy as jnp
from jax import lax
from jax.experimental import pallas as pl
from jax.experimental.pallas import tpu as pltpu
from jax.sharding import PartitionSpec as P

EXP_DEV = 8
LANES = 128
MESH = pl.DeviceIdType.MESH
VMEM = pl.BlockSpec(memory_space=pltpu.VMEM)
SMEM = pl.BlockSpec(memory_space=pltpu.SMEM)
HBM = pl.BlockSpec(memory_space=pltpu.HBM)
epsilon = 1e-06
PAIR = 2
MOST = 8
LAGS = (1, 3, 5, 7, 2, 3, 4, 6)


def chunking(width, relays):
    units = width // (relays * LANES)
    assert units * relays * LANES == width
    count = max(c for c in range(1, MOST + 1) if units % c == 0)
    return count, units // count * LANES


def remote(src, dst, send, recv, device):
    return pltpu.make_async_remote_copy(
        src_ref=src, dst_ref=dst, send_sem=send, recv_sem=recv, device_id=device, device_id_type=MESH
    )


def greet(g, me, d, n):
    barrier = pltpu.get_barrier_semaphore()
    for k in range(1, n):
        pl.semaphore_signal(barrier, inc=1, device_id=(g, lax.rem(me + k, n)), device_id_type=MESH)
    for c in range(1, d):
        pl.semaphore_signal(barrier, inc=1, device_id=(lax.rem(g + c, d), me), device_id_type=MESH)


def meet(d, n):
    pl.semaphore_wait(pltpu.get_barrier_semaphore(), n - 1 + d - 1)


def prepare(routed, probe, gain, normed):
    tokens, width = routed.shape
    probes = probe.shape[1]
    total = jnp.zeros((tokens, LANES), jnp.float32)
    for c in range(width // LANES):
        v = routed[:, c * LANES : (c + 1) * LANES].astype(jnp.float32)
        total = total + v * v
    mean_square = jnp.sum(total, axis=1, keepdims=True) / width
    row = lax.broadcasted_iota(jnp.int32, (tokens, tokens), 0)
    column = lax.broadcasted_iota(jnp.int32, (tokens, tokens), 1)
    flat = jnp.sum(jnp.where(row == column, mean_square, 0.0), axis=0, keepdims=True)
    pick = jnp.where(probe[...] == lax.broadcasted_iota(jnp.int32, (tokens, probes), 0), 1.0, 0.0).T
    scale = lax.rsqrt(jnp.sum(pick * flat, axis=1, keepdims=True) + epsilon)
    pick = pick.astype(jnp.bfloat16)
    step = 512 if width % 512 == 0 else LANES
    for c in range(width // step):
        cols = slice(c * step, (c + 1) * step)
        rows = jnp.dot(pick, routed[:, cols], preferred_element_type=jnp.float32)
        normed[:, cols] = (rows * scale * gain[:, cols].astype(jnp.float32)).astype(jnp.bfloat16)
    return mean_square


def statistics(ids, mean_square, stats):
    tokens, experts = mean_square.shape[0], stats.shape[1]
    lane = lax.broadcasted_iota(jnp.int32, (tokens, experts), 1)
    by_token = ids[...].T
    chosen = jnp.zeros((tokens, experts), jnp.float32)
    for k in range(by_token.shape[1]):
        chosen = chosen + jnp.where(by_token[:, k : k + 1] == lane, 1.0, 0.0)
    stats[0:1, :] = jnp.sum(chosen, axis=0, keepdims=True)
    stats[1:2, :] = jnp.sum(chosen * mean_square, axis=0, keepdims=True)


def inverse(wanted, held, result, n):
    @pl.loop(0, n)
    def _(j):
        value = jnp.int32(0)
        for s in range(n):
            value = value + jnp.where(wanted[j] == held[s], s, 0)
        result[j] = value


def plan(sources, h, half, crossing, pick, cross):
    own, other = h * half, (1 - h) * half
    rank = jnp.int32(0)
    for j in range(half):
        local = sources[own + j] - own
        away = (local < 0) | (local >= half)
        pick[j] = jnp.where(away, half + jnp.minimum(rank, crossing - 1), local)
        rank = rank + jnp.where(away, 1, 0)
    rank = jnp.int32(0)
    found = [jnp.int32(0)] * crossing
    for j in range(half):
        local = sources[other + j] - own
        here = (local >= 0) & (local < half)
        for i in range(min(j + 1, crossing)):
            found[i] = jnp.where(here & (rank == i), local, found[i])
        rank = rank + jnp.where(here, 1, 0)
    for i in range(crossing):
        cross[i] = found[i]


def selection(matrix, table, rows):
    shape = (rows, matrix.shape[1])
    row = lax.broadcasted_iota(jnp.int32, shape, 0)
    column = lax.broadcasted_iota(jnp.int32, shape, 1)
    for j in range(table.shape[0]):
        chosen = column == table[j] * rows + row
        matrix[j * rows : (j + 1) * rows, :] = jnp.where(chosen, 1.0, 0.0).astype(jnp.bfloat16)


def select(matrix, blocks):
    slots, rows, width = blocks.shape
    flat = blocks.astype(jnp.float32).reshape(slots * rows, width).astype(jnp.bfloat16)
    value = jnp.dot(matrix[...], flat, preferred_element_type=jnp.float32)
    return value.reshape(matrix.shape[0] // rows, rows, width).astype(jnp.bfloat16)


def pipeline(count, stages):
    @pl.loop(0, count + max(lag for _, lag in stages))
    def _(t):
        for stage, lag in stages:
            @pl.when((t >= lag) & (t < count + lag))
            def _():
                stage(t - lag)


class Layout:
    def __init__(self, g, me, n, width):
        self.half, self.relays = n // 2, n // 4
        self.count, self.w = chunking(width, self.relays)
        self.wide = self.relays * self.w
        self.pairs = max(1, self.relays // PAIR)
        self.group = self.relays // self.pairs
        self.g, self.me = g, me
        self.h, self.slot = me // self.half, lax.rem(me, self.half)
        self.base = self.h * self.half
        self.r = lax.rem(me, self.relays)
        self.is_relay = me // self.relays == 1 + self.h
        self.outer = self.base + self.h * self.relays
        self.outer_slot = self.h * self.relays
        self.first = (1 + self.h) * self.relays
        self.partner = me + self.relays - 2 * self.relays * self.h
        self.line, self.lane = self.r // self.group, lax.rem(self.r, self.group)

    def piece(self, c, rr, size=1):
        return pl.ds(pl.multiple_of(c * self.wide + rr * self.w, self.w), size * self.w)

    def chunk(self, c):
        return pl.ds(pl.multiple_of(c * self.wide, self.wide), self.wide)


class Route:
    def __init__(self, lay, crossing, take, put, load, store, pick, cross, bufs, sems):
        self.lay, self.crossing, self.take, self.put = lay, crossing, take, put
        self.load, self.store, self.pick, self.cross = load, store, pick, cross
        self.side, self.pool, self.over, self.deal = bufs
        self.ss, self.rs, self.sl, self.rl, self.sf, self.sx, self.rx, self.sg, self.rg = sems

    def direct(self, c, rr):
        l = self.lay
        return remote(
            self.take(c, rr, 1), self.pool.at[c, l.slot], self.ss.at[c, rr], self.rs.at[c, l.slot], (l.g, l.first + rr)
        )

    def direct_in(self, c, s):
        l = self.lay
        return remote(self.take(c, l.r, 1), self.pool.at[c, s], self.ss.at[c, l.r], self.rs.at[c, s], (l.g, l.base + s))

    def sideways(self, c, line):
        l = self.lay
        return remote(
            self.take(c, line * l.group, l.group), self.side.at[c, l.line], self.sl.at[c, line], self.rl.at[c, l.line],
            (l.g, l.outer + line * l.group + l.lane),
        )

    def sideways_in(self, c, line):
        l = self.lay
        return remote(
            self.take(c, line * l.group, l.group), self.side.at[c, line], self.sl.at[c, line], self.rl.at[c, line],
            (l.g, l.outer + line * l.group + l.lane),
        )

    def onward(self, c, line, q):
        l = self.lay
        rr = l.line * l.group + q
        s = l.outer_slot + line * l.group + l.lane
        return remote(
            self.side.at[c, line, :, pl.ds(q * l.w, l.w)], self.pool.at[c, s], self.sf.at[c, line, q],
            self.rs.at[c, s], (l.g, l.first + rr),
        )

    def across(self, c):
        l = self.lay
        return remote(
            self.over.at[c], self.pool.at[c, pl.ds(l.half, self.crossing)], self.sx.at[c], self.rx.at[c], (l.g, l.partner)
        )

    def give(self, c, j):
        l = self.lay
        return remote(self.deal.at[c, j], self.put(c, l.r), self.sg.at[c, j], self.rg.at[c, l.r], (l.g, l.base + j))

    def given(self, c, rr):
        l = self.lay
        return remote(self.deal.at[c, l.slot], self.put(c, rr), self.sg.at[c, l.slot], self.rg.at[c, rr], (l.g, l.first + rr))

    def others(self, stage):
        l = self.lay
        for rr in range(l.relays):
            pl.when(l.first + rr != l.me)(functools.partial(stage, rr))

    def lines(self, stage):
        l = self.lay
        for line in range(l.pairs):
            pl.when(jnp.logical_not(l.is_relay) & (line != l.line))(functools.partial(stage, line))

    def near(self, stage):
        l = self.lay
        for rr in range(l.relays):
            pl.when(jnp.where(l.is_relay, rr != l.r, rr // l.group == l.line))(functools.partial(stage, rr))

    def start_far(self, c):
        self.lines(lambda line: self.sideways(c, line).start())

    def start_near(self, c):
        self.near(lambda rr: self.direct(c, rr).start())

    def forward(self, c):
        l = self.lay

        def stage(line):
            self.sideways_in(c, line).wait_recv()
            for q in range(l.group):
                self.onward(c, line, q).start()

        self.lines(stage)

    def collect(self, c):
        l = self.lay

        @pl.when(l.is_relay)
        def _():
            self.pool[c, l.slot] = self.load(c, l.r)
            for k in range(1, l.half):
                self.direct_in(c, lax.rem(l.slot + k, l.half)).wait_recv()
            self.over[c] = select(self.cross, self.pool[c, : l.half])
            self.across(c).start()

    def hand(self, c):
        l = self.lay

        @pl.when(l.is_relay)
        def _():
            self.across(c).wait_recv()
            self.deal[c] = select(self.pick, self.pool[c])
            for k in range(1, l.half):
                self.give(c, lax.rem(l.slot + k, l.half)).start()
            self.store(c, l.r, self.deal[c, l.slot])

    def arrive(self, c):
        self.others(lambda rr: self.given(c, rr).wait_recv())

    def drain(self, c):
        l = self.lay
        self.near(lambda rr: self.direct(c, rr).wait_send())

        def stage(line):
            self.sideways(c, line).wait_send()
            for q in range(l.group):
                self.onward(c, line, q).wait_send()

        self.lines(stage)

        @pl.when(l.is_relay)
        def _():
            self.across(c).wait_send()
            for k in range(1, l.half):
                self.give(c, lax.rem(l.slot + k, l.half)).wait_send()


def fused_kernel(d, n, crossing, lags, old, new, routed_hbm, ids, probe, gain, gate_hbm, up_hbm, down_hbm, out, totals,
                 wg, wu, wd, routed, normed, x, gate_sum, up_sum, hidden, partial, arrived, summed,
                 stats, st_in, st_mid, st_dp, source, holder, order, crossed, pick, cross, pick2, cross2, sl, sw, sd,
                 sy, ry, ss, rs, ssy, rsy, sz, rz, *rest):
    g, me = lax.axis_index("dp"), lax.axis_index("expert")
    rows, width = normed.shape
    lay = Layout(g, me, n, width)
    count, wide, w = lay.count, lay.wide, lay.w
    chunk, piece = lay.chunk, lay.piece
    tall = d * rows
    down_step = wd.shape[0] // sd.shape[0]

    greet(g, me, d, n)
    load_routed = pltpu.make_async_copy(routed_hbm, routed, sl)
    load_routed.start()
    weights, downs = [], []
    for c in range(count):
        part = pl.ds(c * wide, wide)
        weights.append(pltpu.make_async_copy(gate_hbm.at[part, :], wg.at[part, :], sw.at[0, c]))
        weights.append(pltpu.make_async_copy(up_hbm.at[part, :], wu.at[part, :], sw.at[1, c]))
    for p in range(sd.shape[0]):
        part = pl.ds(p * down_step, down_step)
        downs.append(pltpu.make_async_copy(down_hbm.at[part, :], wd.at[part, :], sd.at[p]))
    inverse(old, new, source, n)
    inverse(new, old, holder, n)
    for places, picks, crosses in ((source, pick, cross), (holder, pick2, cross2)):
        plan(places, lay.h, lay.half, crossing, order, crossed)
        selection(picks, order, rows)
        selection(crosses, crossed, rows)
    load_routed.wait()
    for load in weights + downs:
        load.start()
    mean_square = prepare(routed, probe, gain, normed)
    meet(d, n)

    def put_x(c, rr, value):
        x[g, :, piece(c, rr)] = value

    def put_out(c, rr, value):
        out[:, piece(c, rr)] = value

    there = Route(
        lay, crossing,
        lambda c, rr, size: normed.at[:, piece(c, rr, size)], lambda c, rr: x.at[g, :, piece(c, rr)],
        lambda c, rr: normed[:, piece(c, rr)], put_x, pick, cross, rest[0:4], rest[8:17],
    )
    summed_piece = lambda rr, size: pl.ds(pl.multiple_of(rr * w, w), size * w)
    home = Route(
        lay, crossing,
        lambda c, rr, size: summed.at[c, :, summed_piece(rr, size)], lambda c, rr: out.at[:, piece(c, rr)],
        lambda c, rr: summed[c, :, summed_piece(rr, 1)], put_out, pick2, cross2, rest[4:8], rest[17:26],
    )

    def along(c, q):
        here = x.at[g, :, chunk(c)]
        return remote(here, here, sy.at[c, q], ry.at[c, g], (lax.rem(g + q, d), me))

    def along_in(c, q):
        f = lax.rem(g + d - q, d)
        other = x.at[f, :, chunk(c)]
        return remote(other, other, sy.at[c, q], ry.at[c, f], (f, me))

    def stat(k):
        return remote(stats, st_in.at[me], ss.at[k], rs.at[me], (g, lax.rem(me + k, n)))

    def stat_in(k):
        s = lax.rem(me + n - k, n)
        return remote(stats, st_in.at[s], ss.at[k], rs.at[s], (g, s))

    def stat_dp(q):
        return remote(st_mid, st_dp.at[g], ssy.at[q], rsy.at[g], (lax.rem(g + q, d), me))

    ahead = min(2, count)
    pl.loop(0, count)(there.start_far)
    pl.loop(0, ahead)(there.start_near)
    pl.when(lay.is_relay)(lambda: pl.loop(ahead, count)(there.start_near))

    statistics(ids, mean_square, stats)
    for k in range(1, n):
        stat(k).start()
    st_in[me] = stats[...]
    gate_sum[...] = jnp.zeros_like(gate_sum)
    up_sum[...] = jnp.zeros_like(up_sum)

    def forward(c):
        there.forward(c)
        pl.when(jnp.logical_not(lay.is_relay) & (c + ahead < count))(lambda: there.start_near(c + ahead))

    def take(c):
        there.arrive(c)
        for q in range(1, d):
            along(c, q).start()

    def absorb(c):
        for q in range(1, d):
            along_in(c, q).wait_recv()
        part = x[:, :, chunk(c)].astype(jnp.float32).reshape(tall, wide).astype(jnp.bfloat16)
        for k, (hbm, ref, total) in enumerate(((gate_hbm, wg, gate_sum), (up_hbm, wu, up_sum))):
            pltpu.make_async_copy(hbm.at[chunk(c), :], ref.at[chunk(c), :], sw.at[k, c]).wait()
            total[...] += jnp.dot(part, ref[chunk(c), :], preferred_element_type=jnp.float32)

    pipeline(count, [
        (forward, 0), (there.collect, lags[0]), (there.hand, lags[1]), (take, lags[2]), (absorb, lags[3]),
    ])

    gate = gate_sum[...]
    hidden[...] = (gate / (1.0 + jnp.exp(-gate)) * up_sum[...]).astype(jnp.bfloat16)
    for load in downs:
        load.wait()

    def home_copy(c, q):
        t = lax.rem(g + q, d)
        return remote(partial.at[c, t], arrived.at[c, g], sz.at[c, q], rz.at[c, g], (t, me))

    def home_in(c, q):
        f = lax.rem(g + d - q, d)
        return remote(partial.at[c, f], arrived.at[c, f], sz.at[c, q], rz.at[c, f], (f, me))

    def make(c):
        value = jnp.dot(hidden[...], wd[:, chunk(c)], preferred_element_type=jnp.float32)
        partial[c] = value.reshape(d, rows, wide).astype(jnp.bfloat16)
        for q in range(1, d):
            home_copy(c, q).start()

    def add(c):
        for q in range(1, d):
            home_in(c, q).wait_recv()
        total = partial[c, g].astype(jnp.float32)
        for q in range(1, d):
            total = total + arrived[c, lax.rem(g + q, d)].astype(jnp.float32)
        summed[c] = total.astype(jnp.bfloat16)
        home.start_far(c)
        home.start_near(c)

    for k in range(1, n):
        stat_in(k).wait_recv()
    mid = st_in[0]
    for s in range(1, n):
        mid = mid + st_in[s]
    st_mid[...] = mid
    st_dp[g] = mid
    for q in range(1, d):
        stat_dp(q).start()

    pipeline(count, [
        (make, 0), (add, lags[4]), (home.forward, lags[5]), (home.collect, lags[6]), (home.hand, lags[7]),
    ])

    for q in range(1, d):
        f = lax.rem(g + d - q, d)
        remote(st_mid, st_dp.at[f], ssy.at[q], rsy.at[f], (f, me)).wait_recv()
    total = st_dp[0]
    for f in range(1, d):
        total = total + st_dp[f]
    totals[...] = total

    for k in range(1, n):
        stat(k).wait_send()
    for q in range(1, d):
        stat_dp(q).wait_send()

    @pl.loop(0, count)
    def _(c):
        there.drain(c)
        home.drain(c)
        for q in range(1, d):
            along(c, q).wait_send()
            home_copy(c, q).wait_send()

    pl.loop(0, count)(home.arrive)


def fused(crossing, collective, d, n, experts, old, new, routed, ids, probe, gain, gate, up, down):
    tokens, width = routed.shape
    rows = probe.shape[1]
    units = gate.shape[1]
    lay = Layout(0, 0, n, width)
    count, w, half, relays, pairs, group = lay.count, lay.w, lay.half, lay.relays, lay.pairs, lay.group
    full = lay.wide
    dma = pltpu.SemaphoreType.DMA
    block = lambda *shape: pltpu.VMEM(shape, jnp.bfloat16)
    wide = lambda *shape: pltpu.VMEM(shape, jnp.float32)
    numbers = lambda size: pltpu.SMEM((size,), jnp.int32)
    matrices = [block(half * rows, (half + crossing) * rows), block(crossing * rows, half * rows)]
    bufs = [
        block(count, pairs, rows, group * w), block(count, half + crossing, rows, w),
        block(count, crossing, rows, w), block(count, half, rows, w),
    ]
    sems = [
        dma((count, relays)), dma((count, half)), dma((count, pairs)), dma((count, pairs)), dma((count, pairs, group)),
        dma((count,)), dma((count,)), dma((count, half)), dma((count, relays)),
    ]
    return pl.pallas_call(
        functools.partial(fused_kernel, d, n, crossing, LAGS),
        out_shape=(
            jax.ShapeDtypeStruct((rows, width), jnp.bfloat16),
            jax.ShapeDtypeStruct((2, experts), jnp.float32),
        ),
        in_specs=[SMEM, SMEM, HBM, VMEM, VMEM, VMEM, HBM, HBM, HBM],
        out_specs=(VMEM, VMEM),
        scratch_shapes=[
            block(width, units), block(width, units), block(units, width),
            block(tokens, width), block(rows, width), block(d, rows, width),
            wide(d * rows, units), wide(d * rows, units), block(d * rows, units),
            block(count, d, rows, full), block(count, d, rows, full), block(count, rows, full),
            wide(2, experts), wide(n, 2, experts), wide(2, experts), wide(d, 2, experts),
            numbers(n), numbers(n), numbers(half), numbers(crossing), *matrices, *matrices,
            dma, dma((2, count)), dma((8,)),
            dma((count, d)), dma((count, d)), dma((n,)), dma((n,)), dma((d,)), dma((d,)),
            dma((count, d)), dma((count, d)),
            *bufs, *bufs, *sems, *sems,
        ],
        compiler_params=pltpu.CompilerParams(
            collective_id=collective, has_side_effects=True, vmem_limit_bytes=62 << 20
        ),
    )(old, new, routed, ids, probe, gain, gate, up, down)


def on_device(
    routed,
    expert_ids,
    norm_gain,
    gate_weight,
    up_weight,
    down_weight,
    old_place,
    new_place,
    probe_ids,
):
    n, d = lax.axis_size("expert"), lax.axis_size("dp")
    experts = EXP_DEV * n
    tokens = routed.shape[0] * d * n
    half = n // 2
    widths = (half // 2, half * 5 // 8, half)
    index = jnp.arange(n, dtype=jnp.int32)
    apart = (index[:, None] < half) & (index[None, :] >= half)
    crossings = jnp.sum(((old_place[:, None] == new_place[None, :]) & apart).astype(jnp.int32))
    branch = (crossings > widths[0]).astype(jnp.int32) + (crossings > widths[1]).astype(jnp.int32)
    kernels = [functools.partial(fused, widths[i], i, d, n, experts) for i in range(3)]
    probe_out, totals = lax.switch(
        branch, kernels,
        old_place, new_place, routed, expert_ids.T, probe_ids.reshape(1, -1), norm_gain.reshape(1, -1),
        gate_weight[0], up_weight[0], down_weight[0],
    )
    owned = lax.dynamic_slice_in_dim(totals, lax.axis_index("expert") * EXP_DEV, EXP_DEV, 1)
    expert_load = owned[0] * experts / (tokens * expert_ids.shape[1])
    expert_energy = owned[1] / owned[0]
    return (expert_load, expert_energy, probe_out)


def solution(mesh):
    in_specs = (
        P(("dp", "expert"), None),
        P(("dp", "expert"), None),
        P(),
        P("expert", None, "dp"),
        P("expert", None, "dp"),
        P("expert", "dp", None),
        P(),
        P(),
        P(("dp", "expert")),
    )
    out_specs = (P("expert"), P("expert"), P(("dp", "expert"), None))
    return jax.shard_map(
        on_device, mesh=mesh, in_specs=in_specs, out_specs=out_specs, check_vma=False
    )
```

```python
import functools

import jax
import jax.numpy as jnp
from jax import lax
from jax.experimental import pallas as pl
from jax.experimental.pallas import tpu as pltpu
from jax.sharding import PartitionSpec as P

EXP_DEV = 8
LANES = 128
MESH = pl.DeviceIdType.MESH
VMEM = pl.BlockSpec(memory_space=pltpu.VMEM)
SMEM = pl.BlockSpec(memory_space=pltpu.SMEM)
HBM = pl.BlockSpec(memory_space=pltpu.HBM)
epsilon = 1e-06
PAIR = 2
AHEAD = 4
EARLY = (3, 3)
MOST = 14
LAGS = {7: (2, 4, 6, 1, 2, 4, 6), 14: (4, 8, 12, 3, 5, 7, 10)}


def chunking(width, relays):
    units = width // (relays * LANES)
    assert units * relays * LANES == width
    count = max(c for c in range(1, MOST + 1) if units % c == 0)
    return count, units // count * LANES


def remote(src, dst, send, recv, device):
    return pltpu.make_async_remote_copy(
        src_ref=src, dst_ref=dst, send_sem=send, recv_sem=recv, device_id=device, device_id_type=MESH
    )


def greet(g, me, d, n):
    barrier = pltpu.get_barrier_semaphore()
    for k in range(1, n):
        pl.semaphore_signal(barrier, inc=1, device_id=(g, lax.rem(me + k, n)), device_id_type=MESH)
    for c in range(1, d):
        pl.semaphore_signal(barrier, inc=1, device_id=(lax.rem(g + c, d), me), device_id_type=MESH)


def meet(d, n):
    pl.semaphore_wait(pltpu.get_barrier_semaphore(), n - 1 + d - 1)


def prepare(routed, probe, gain, normed):
    tokens, width = routed.shape
    probes = probe.shape[1]
    total = jnp.zeros((tokens, LANES), jnp.float32)
    for c in range(width // LANES):
        v = routed[:, c * LANES : (c + 1) * LANES].astype(jnp.float32)
        total = total + v * v
    mean_square = jnp.sum(total, axis=1, keepdims=True) / width
    row = lax.broadcasted_iota(jnp.int32, (tokens, tokens), 0)
    column = lax.broadcasted_iota(jnp.int32, (tokens, tokens), 1)
    flat = jnp.sum(jnp.where(row == column, mean_square, 0.0), axis=0, keepdims=True)
    pick = jnp.where(probe[...] == lax.broadcasted_iota(jnp.int32, (tokens, probes), 0), 1.0, 0.0).T
    scale = lax.rsqrt(jnp.sum(pick * flat, axis=1, keepdims=True) + epsilon)
    pick = pick.astype(jnp.bfloat16)
    step = 512 if width % 512 == 0 else LANES
    for c in range(width // step):
        cols = slice(c * step, (c + 1) * step)
        rows = jnp.dot(pick, routed[:, cols], preferred_element_type=jnp.float32)
        normed[:, cols] = (rows * scale * gain[:, cols].astype(jnp.float32)).astype(jnp.bfloat16)
    return mean_square


def statistics(ids, mean_square, stats):
    tokens, experts = mean_square.shape[0], stats.shape[1]
    lane = lax.broadcasted_iota(jnp.int32, (tokens, experts), 1)
    by_token = ids[...].T
    chosen = jnp.zeros((tokens, experts), jnp.float32)
    for k in range(by_token.shape[1]):
        chosen = chosen + jnp.where(by_token[:, k : k + 1] == lane, 1.0, 0.0)
    stats[0:1, :] = jnp.sum(chosen, axis=0, keepdims=True)
    stats[1:2, :] = jnp.sum(chosen * mean_square, axis=0, keepdims=True)


def inverse(wanted, held, result, n):
    @pl.loop(0, n)
    def _(j):
        value = jnp.int32(0)
        for s in range(n):
            value = value + jnp.where(wanted[j] == held[s], s, 0)
        result[j] = value


def plan(sources, h, half, crossing, pick, cross):
    own, other = h * half, (1 - h) * half
    rank = jnp.int32(0)
    for j in range(half):
        local = sources[own + j] - own
        away = (local < 0) | (local >= half)
        pick[j] = jnp.where(away, half + jnp.minimum(rank, crossing - 1), local)
        rank = rank + jnp.where(away, 1, 0)
    rank = jnp.int32(0)
    found = [jnp.int32(0)] * crossing
    for j in range(half):
        local = sources[other + j] - own
        here = (local >= 0) & (local < half)
        for i in range(min(j + 1, crossing)):
            found[i] = jnp.where(here & (rank == i), local, found[i])
        rank = rank + jnp.where(here, 1, 0)
    for i in range(crossing):
        cross[i] = found[i]


def selection(matrix, table, rows):
    shape = (rows, matrix.shape[1])
    row = lax.broadcasted_iota(jnp.int32, shape, 0)
    column = lax.broadcasted_iota(jnp.int32, shape, 1)
    for j in range(table.shape[0]):
        chosen = column == table[j] * rows + row
        matrix[j * rows : (j + 1) * rows, :] = jnp.where(chosen, 1.0, 0.0).astype(jnp.bfloat16)


def select(matrix, blocks):
    slots, rows, width = blocks.shape
    flat = blocks.astype(jnp.float32).reshape(slots * rows, width).astype(jnp.bfloat16)
    value = jnp.dot(matrix[...], flat, preferred_element_type=jnp.float32)
    return value.reshape(matrix.shape[0] // rows, rows, width).astype(jnp.bfloat16)


def pipeline(count, stages):
    @pl.loop(0, count + max(lag for _, lag in stages))
    def _(t):
        for stage, lag in stages:
            @pl.when((t >= lag) & (t < count + lag))
            def _():
                stage(t - lag)


class Layout:
    def __init__(self, g, me, n, width):
        self.half, self.relays = n // 2, n // 4
        self.count, self.w = chunking(width, self.relays)
        self.wide = self.relays * self.w
        self.pairs = max(1, self.relays // PAIR)
        self.group = self.relays // self.pairs
        self.g, self.me = g, me
        self.h, self.slot = me // self.half, lax.rem(me, self.half)
        self.base = self.h * self.half
        self.r = lax.rem(me, self.relays)
        self.is_relay = me // self.relays == 1 + self.h
        self.outer = self.base + self.h * self.relays
        self.outer_slot = self.h * self.relays
        self.first = (1 + self.h) * self.relays
        self.partner = me + self.relays - 2 * self.relays * self.h
        self.line, self.lane = self.r // self.group, lax.rem(self.r, self.group)

    def piece(self, c, rr, size=1):
        return pl.ds(pl.multiple_of(c * self.wide + rr * self.w, self.w), size * self.w)

    def chunk(self, c):
        return pl.ds(pl.multiple_of(c * self.wide, self.wide), self.wide)


class Route:
    def __init__(self, lay, crossing, early, take, put, load, store, pick, cross, bufs, sems):
        self.lay, self.crossing, self.take, self.put = lay, crossing, take, put
        self.load, self.store, self.pick, self.cross = load, store, pick, cross
        self.side, self.pool, self.over, self.deal = bufs
        self.s_direct, self.s_early, self.s_side, self.s_onward, self.s_across, self.s_give = sems[:6]
        self.r_direct, self.r_side, self.r_across, self.r_give = sems[6:]
        self.early = early

    def several(self, ref, send, recv):
        return remote(ref, ref, send, recv, (self.lay.g, self.lay.partner))

    def direct(self, c, rr, send):
        l = self.lay
        return remote(self.take(c, rr, 1), self.pool.at[c, l.slot], send, self.r_direct.at[c], (l.g, l.first + rr))

    def sideways(self, c, line):
        l = self.lay
        return remote(
            self.take(c, line * l.group, l.group), self.side.at[c, l.line], self.s_side, self.r_side.at[c],
            (l.g, l.outer + line * l.group + l.lane),
        )

    def onward(self, c, line, q):
        l = self.lay
        return remote(
            self.side.at[c, line, :, pl.ds(q * l.w, l.w)], self.pool.at[c, l.outer_slot + line * l.group + l.lane],
            self.s_onward, self.r_direct.at[c], (l.g, l.first + l.line * l.group + q),
        )

    def across(self, c):
        l = self.lay
        return remote(
            self.over.at[c], self.pool.at[c, pl.ds(l.half, self.crossing)], self.s_across, self.r_across.at[c], (l.g, l.partner)
        )

    def give(self, c, j):
        l = self.lay
        return remote(self.deal.at[c, j], self.put(c, l.r, 1), self.s_give, self.r_give.at[c], (l.g, l.base + j))

    def lines(self, stage):
        l = self.lay
        for line in range(l.pairs):
            pl.when(jnp.logical_not(l.is_relay) & (line != l.line))(functools.partial(stage, line))

    def start_far(self, c):
        def stage(line):
            @pl.when(c >= self.early)
            def _():
                self.sideways(c, line).start()

            @pl.when(c < self.early)
            def _():
                for q in range(self.lay.group):
                    self.direct(c, line * self.lay.group + q, self.s_early).start()

        self.lines(stage)

    def start_near(self, c):
        l = self.lay
        for rr in range(l.relays):
            near = jnp.where(l.is_relay, rr != l.r, rr // l.group == l.line)
            pl.when(near)(lambda rr=rr: self.direct(c, rr, self.s_direct).start())

    def forward(self, c):
        l = self.lay

        def stage(line):
            for q in range(l.group):
                self.onward(c, line, q).start()

        if l.pairs > 1:
            @pl.when(jnp.logical_not(l.is_relay) & (c >= self.early))
            def _():
                self.several(self.side.at[c, pl.ds(0, l.pairs - 1)], self.s_side, self.r_side.at[c]).wait_recv()
                self.lines(stage)

    def collect(self, c):
        l = self.lay

        @pl.when(l.is_relay)
        def _():
            self.pool[c, l.slot] = self.load(c, l.r)
            self.several(self.pool.at[c, pl.ds(0, l.half - 1)], self.s_direct, self.r_direct.at[c]).wait_recv()
            self.over[c] = select(self.cross, self.pool[c, : l.half])
            self.across(c).start()

    def hand(self, c):
        l = self.lay

        @pl.when(l.is_relay)
        def _():
            self.across(c).wait_recv()
            self.deal[c] = select(self.pick, self.pool[c])
            for k in range(1, l.half):
                self.give(c, lax.rem(l.slot + k, l.half)).start()
            self.store(c, l.r, self.deal[c, l.slot])

    def arrive(self, c):
        l = self.lay

        @pl.when(l.is_relay)
        def _():
            self.several(self.put(c, 0, l.relays - 1), self.s_give, self.r_give.at[c]).wait_recv()

        @pl.when(jnp.logical_not(l.is_relay))
        def _():
            self.several(self.put(c, 0, l.relays), self.s_give, self.r_give.at[c]).wait_recv()

    def drain(self):
        l = self.lay

        @pl.when(l.is_relay)
        def _():
            self.several(self.pool.at[:, pl.ds(0, l.relays - 1)], self.s_direct, self.r_direct.at[0]).wait_send()
            self.several(self.over, self.s_across, self.r_across.at[0]).wait_send()
            self.several(self.deal.at[:, pl.ds(0, l.half - 1)], self.s_give, self.r_give.at[0]).wait_send()

        @pl.when(jnp.logical_not(l.is_relay))
        def _():
            self.several(self.pool.at[:, pl.ds(0, l.group)], self.s_direct, self.r_direct.at[0]).wait_send()
            if l.pairs > 1:
                sent = self.side.at[pl.ds(self.early, l.count - self.early), pl.ds(0, l.pairs - 1)]
                if self.early:
                    first = self.pool.at[pl.ds(0, self.early), pl.ds(0, l.relays - l.group)]
                    self.several(first, self.s_early, self.r_side.at[0]).wait_send()
                self.several(sent, self.s_side, self.r_side.at[0]).wait_send()
                self.several(sent, self.s_onward, self.r_side.at[0]).wait_send()


def fused_kernel(d, n, crossing, old, new, routed_hbm, ids, probe, gain, gate_hbm, up_hbm, down_hbm, out, totals,
                 wg, wu, wd, routed, normed, x, gate_sum, up_sum, hidden, partial, arrived, summed,
                 stats, st_in, st_mid, st_dp, source, holder, order, crossed, pick, cross, pick2, cross2, sl, sw, sd,
                 sy, ry, ss, rs, ssy, rsy, sz, rz, *rest):
    g, me = lax.axis_index("dp"), lax.axis_index("expert")
    rows, width = normed.shape
    lay = Layout(g, me, n, width)
    count, wide, w = lay.count, lay.wide, lay.w
    chunk, piece = lay.chunk, lay.piece
    tall = d * rows
    down_parts = 8
    down_step = wd.shape[0] // down_parts

    load_routed = pltpu.make_async_copy(routed_hbm, routed, sl)
    load_routed.start()
    greet(g, me, d, n)
    weights, downs = [], []
    for c in range(count):
        part = pl.ds(c * wide, wide)
        weights.append(pltpu.make_async_copy(gate_hbm.at[part, :], wg.at[part, :], sw.at[c]))
        weights.append(pltpu.make_async_copy(up_hbm.at[part, :], wu.at[part, :], sw.at[c]))
    for p in range(down_parts):
        part = pl.ds(p * down_step, down_step)
        downs.append(pltpu.make_async_copy(down_hbm.at[part, :], wd.at[part, :], sd))
    load_routed.wait()
    for load in weights + downs:
        load.start()
    mean_square = prepare(routed, probe, gain, normed)
    meet(d, n)

    def put_x(c, rr, value):
        x[g, :, piece(c, rr)] = value

    def put_out(c, rr, value):
        out[:, piece(c, rr)] = value

    there = Route(
        lay, crossing, min(EARLY[0], count - 1),
        lambda c, rr, size: normed.at[:, piece(c, rr, size)], lambda c, rr, size: x.at[g, :, piece(c, rr, size)],
        lambda c, rr: normed[:, piece(c, rr)], put_x, pick, cross, rest[0:4], rest[8:18],
    )
    summed_piece = lambda rr, size: pl.ds(pl.multiple_of(rr * w, w), size * w)
    home = Route(
        lay, crossing, min(EARLY[1], count - 1),
        lambda c, rr, size: summed.at[c, :, summed_piece(rr, size)], lambda c, rr, size: out.at[:, piece(c, rr, size)],
        lambda c, rr: summed[c, :, summed_piece(rr, 1)], put_out, pick2, cross2, rest[4:8], rest[18:28],
    )

    def peers(ref, send, recv):
        return remote(ref, ref, send, recv, (lax.rem(g + 1, d), me))

    def along(c, q):
        here = x.at[g, :, chunk(c)]
        return remote(here, here, sy, ry.at[c], (lax.rem(g + q, d), me))

    def stat(k):
        return remote(stats, st_in.at[me], ss, rs, (g, lax.rem(me + k, n)))

    def stat_all():
        part = st_in.at[pl.ds(0, n - 1)]
        return remote(part, part, ss, rs, (g, lay.partner))

    def stat_dp(q):
        return remote(st_mid, st_dp.at[g], ssy, rsy, (lax.rem(g + q, d), me))

    ahead = min(AHEAD, count)
    pl.loop(0, count)(there.start_far)
    pl.loop(0, ahead)(there.start_near)
    pl.when(lay.is_relay)(lambda: pl.loop(ahead, count)(there.start_near))

    @pl.when(jnp.logical_not(lay.is_relay))
    def _():
        @pl.loop(0, count)
        def _(c):
            there.forward(c)
            pl.when(c + ahead < count)(lambda: there.start_near(c + ahead))

    inverse(old, new, source, n)
    inverse(new, old, holder, n)
    for places, picks, crosses in ((source, pick, cross), (holder, pick2, cross2)):
        plan(places, lay.h, lay.half, crossing, order, crossed)
        selection(picks, order, rows)
        selection(crosses, crossed, rows)
    statistics(ids, mean_square, stats)
    for k in range(1, n):
        stat(k).start()
    st_in[me] = stats[...]
    gate_sum[...] = jnp.zeros_like(gate_sum)
    up_sum[...] = jnp.zeros_like(up_sum)

    def take(c):
        there.arrive(c)
        for q in range(1, d):
            along(c, q).start()

    def absorb(c):
        if d > 1:
            peers(x.at[pl.ds(0, d - 1), :, chunk(c)], sy, ry.at[c]).wait_recv()
        part = x[:, :, chunk(c)].astype(jnp.float32).reshape(tall, wide).astype(jnp.bfloat16)
        both = pl.ds(0, 2 * wide)
        pltpu.make_async_copy(gate_hbm.at[both, :], wg.at[both, :], sw.at[c]).wait()
        for ref, total in ((wg, gate_sum), (wu, up_sum)):
            total[...] += jnp.dot(part, ref[chunk(c), :], preferred_element_type=jnp.float32)

    lags = LAGS[count]
    pipeline(count, [(there.collect, 0), (there.hand, lags[0]), (take, lags[1]), (absorb, lags[2])])

    gate = gate_sum[...]
    hidden[...] = (gate / (1.0 + jnp.exp(-gate)) * up_sum[...]).astype(jnp.bfloat16)
    pltpu.make_async_copy(down_hbm, wd, sd).wait()

    def home_copy(c, q):
        return remote(partial.at[c, lax.rem(g + q, d)], arrived.at[c, q - 1], sz, rz.at[c], (lax.rem(g + q, d), me))

    def make(c):
        value = jnp.dot(hidden[...], wd[:, chunk(c)], preferred_element_type=jnp.float32)
        partial[c] = value.reshape(d, rows, wide).astype(jnp.bfloat16)
        for q in range(1, d):
            home_copy(c, q).start()

    def add(c):
        total = partial[c, g].astype(jnp.float32)
        if d > 1:
            peers(arrived.at[c], sz, rz.at[c]).wait_recv()
        for q in range(1, d):
            total = total + arrived[c, q - 1].astype(jnp.float32)
        summed[c] = total.astype(jnp.bfloat16)
        home.start_far(c)
        home.start_near(c)

    stat_all().wait_recv()
    mid = st_in[0]
    for s in range(1, n):
        mid = mid + st_in[s]
    st_mid[...] = mid
    st_dp[g] = mid
    for q in range(1, d):
        stat_dp(q).start()

    pipeline(count, [
        (make, 0), (add, lags[3]), (home.forward, lags[4]), (home.collect, lags[5]), (home.hand, lags[6]),
    ])

    stat_all().wait_send()
    if d > 1:
        peers(st_dp.at[pl.ds(0, d - 1)], ssy, rsy).wait()
        peers(x.at[pl.ds(0, d - 1)], sy, ry.at[0]).wait_send()
        peers(arrived, sz, rz.at[0]).wait_send()
    total = st_dp[0]
    for f in range(1, d):
        total = total + st_dp[f]
    totals[...] = total

    there.drain()
    home.drain()
    pl.loop(0, count)(home.arrive)


def fused(crossing, collective, d, n, experts, old, new, routed, ids, probe, gain, gate, up, down):
    tokens, width = routed.shape
    rows = probe.shape[1]
    units = gate.shape[1]
    lay = Layout(0, 0, n, width)
    count, w, half, relays, pairs, group = lay.count, lay.w, lay.half, lay.relays, lay.pairs, lay.group
    full = lay.wide
    dma = pltpu.SemaphoreType.DMA
    block = lambda *shape: pltpu.VMEM(shape, jnp.bfloat16)
    wide = lambda *shape: pltpu.VMEM(shape, jnp.float32)
    numbers = lambda size: pltpu.SMEM((size,), jnp.int32)
    matrices = [block(half * rows, (half + crossing) * rows), block(crossing * rows, half * rows)]
    bufs = [
        block(count, pairs, rows, group * w), block(count, half + crossing, rows, w),
        block(count, crossing, rows, w), block(count, half, rows, w),
    ]
    sems = [dma, dma, dma, dma, dma, dma, dma((count,)), dma((count,)), dma((count,)), dma((count,))]
    return pl.pallas_call(
        functools.partial(fused_kernel, d, n, crossing),
        out_shape=(
            jax.ShapeDtypeStruct((rows, width), jnp.bfloat16),
            jax.ShapeDtypeStruct((2, experts), jnp.float32),
        ),
        in_specs=[SMEM, SMEM, HBM, VMEM, VMEM, VMEM, HBM, HBM, HBM],
        out_specs=(VMEM, VMEM),
        scratch_shapes=[
            block(width, units), block(width, units), block(units, width),
            block(tokens, width), block(rows, width), block(d, rows, width),
            wide(d * rows, units), wide(d * rows, units), block(d * rows, units),
            block(count, d, rows, full), block(count, max(1, d - 1), rows, full), block(count, rows, full),
            wide(2, experts), wide(n, 2, experts), wide(2, experts), wide(d, 2, experts),
            numbers(n), numbers(n), numbers(half), numbers(crossing), *matrices, *matrices,
            dma, dma((count,)), dma,
            dma, dma((count,)), dma, dma, dma, dma, dma, dma((count,)),
            *bufs, *bufs, *sems, *sems,
        ],
        compiler_params=pltpu.CompilerParams(
            collective_id=collective, has_side_effects=True, vmem_limit_bytes=125 << 19
        ),
    )(old, new, routed, ids, probe, gain, gate, up, down)


def on_device(
    routed,
    expert_ids,
    norm_gain,
    gate_weight,
    up_weight,
    down_weight,
    old_place,
    new_place,
    probe_ids,
):
    n, d = lax.axis_size("expert"), lax.axis_size("dp")
    experts = EXP_DEV * n
    tokens = routed.shape[0] * d * n
    half = n // 2
    widths = (half // 2, half * 5 // 8, half)
    index = jnp.arange(n, dtype=jnp.int32)
    apart = (index[:, None] < half) & (index[None, :] >= half)
    crossings = jnp.sum(((old_place[:, None] == new_place[None, :]) & apart).astype(jnp.int32))
    branch = (crossings > widths[0]).astype(jnp.int32) + (crossings > widths[1]).astype(jnp.int32)
    kernels = [functools.partial(fused, widths[i], i, d, n, experts) for i in range(3)]
    probe_out, totals = lax.switch(
        branch, kernels,
        old_place, new_place, routed, expert_ids.T, probe_ids.reshape(1, -1), norm_gain.reshape(1, -1),
        gate_weight[0], up_weight[0], down_weight[0],
    )
    owned = lax.dynamic_slice_in_dim(totals, lax.axis_index("expert") * EXP_DEV, EXP_DEV, 1)
    expert_load = owned[0] * experts / (tokens * expert_ids.shape[1])
    expert_energy = owned[1] / owned[0]
    return (expert_load, expert_energy, probe_out)


def solution(mesh):
    in_specs = (
        P(("dp", "expert"), None),
        P(("dp", "expert"), None),
        P(),
        P("expert", None, "dp"),
        P("expert", None, "dp"),
        P("expert", "dp", None),
        P(),
        P(),
        P(("dp", "expert")),
    )
    out_specs = (P("expert"), P("expert"), P(("dp", "expert"), None))
    return jax.shard_map(
        on_device, mesh=mesh, in_specs=in_specs, out_specs=out_specs, check_vma=False
    )
```

```python
import functools

import jax
import jax.numpy as jnp
from jax import lax
from jax.experimental import pallas as pl
from jax.experimental.pallas import tpu as pltpu
from jax.sharding import PartitionSpec as P

EXP_DEV = 8
LANES = 128
MESH = pl.DeviceIdType.MESH
VMEM = pl.BlockSpec(memory_space=pltpu.VMEM)
SMEM = pl.BlockSpec(memory_space=pltpu.SMEM)
HBM = pl.BlockSpec(memory_space=pltpu.HBM)
epsilon = 1e-06
PAIR = 2
AHEAD = 4
FIRST = (4, 0)
SECOND = (7, 3)
MOST = 14
LAGS = {7: (2, 4, 6, 2, 3, 4, 6), 14: (4, 7, 11, 4, 6, 8, 11)}


def chunking(width, relays):
    units = width // (relays * LANES)
    assert units * relays * LANES == width
    count = max(c for c in range(1, MOST + 1) if units % c == 0)
    return count, units // count * LANES


def direct_chunks(count, wanted):
    early = min(wanted[0], count // 2)
    return early, min(wanted[1], count // 4)


def remote(src, dst, send, recv, device):
    return pltpu.make_async_remote_copy(
        src_ref=src, dst_ref=dst, send_sem=send, recv_sem=recv, device_id=device, device_id_type=MESH
    )


def greet(g, me, d, n):
    barrier = pltpu.get_barrier_semaphore()
    for k in range(1, n):
        pl.semaphore_signal(barrier, inc=1, device_id=(g, lax.rem(me + k, n)), device_id_type=MESH)
    for c in range(1, d):
        pl.semaphore_signal(barrier, inc=1, device_id=(lax.rem(g + c, d), me), device_id_type=MESH)


def meet(d, n):
    pl.semaphore_wait(pltpu.get_barrier_semaphore(), n - 1 + d - 1)


def prepare(routed, probe, gain, normed):
    tokens, width = routed.shape
    probes = probe.shape[1]
    total = jnp.zeros((tokens, LANES), jnp.float32)
    for c in range(width // LANES):
        v = routed[:, c * LANES : (c + 1) * LANES].astype(jnp.float32)
        total = total + v * v
    mean_square = jnp.sum(total, axis=1, keepdims=True) / width
    row = lax.broadcasted_iota(jnp.int32, (tokens, tokens), 0)
    column = lax.broadcasted_iota(jnp.int32, (tokens, tokens), 1)
    flat = jnp.sum(jnp.where(row == column, mean_square, 0.0), axis=0, keepdims=True)
    pick = jnp.where(probe[...] == lax.broadcasted_iota(jnp.int32, (tokens, probes), 0), 1.0, 0.0).T
    scale = lax.rsqrt(jnp.sum(pick * flat, axis=1, keepdims=True) + epsilon)
    pick = pick.astype(jnp.bfloat16)
    step = 512 if width % 512 == 0 else LANES
    for c in range(width // step):
        cols = slice(c * step, (c + 1) * step)
        rows = jnp.dot(pick, routed[:, cols], preferred_element_type=jnp.float32)
        normed[:, cols] = (rows * scale * gain[cols].astype(jnp.float32)[None, :]).astype(jnp.bfloat16)
    return mean_square


def statistics(ids, mean_square, stats):
    tokens, experts = mean_square.shape[0], stats.shape[1]
    lane = lax.broadcasted_iota(jnp.int32, (tokens, experts), 1)
    by_token = ids[...].T
    chosen = jnp.zeros((tokens, experts), jnp.float32)
    for k in range(by_token.shape[1]):
        chosen = chosen + jnp.where(by_token[:, k : k + 1] == lane, 1.0, 0.0)
    stats[0:1, :] = jnp.sum(chosen, axis=0, keepdims=True)
    stats[1:2, :] = jnp.sum(chosen * mean_square, axis=0, keepdims=True)


def inverse(wanted, held, result, n):
    @pl.loop(0, n)
    def _(j):
        value = jnp.int32(0)
        for s in range(n):
            value = value + jnp.where(wanted[j] == held[s], s, 0)
        result[j] = value


def plan(sources, h, half, crossing, pick, cross):
    own, other = h * half, (1 - h) * half
    rank = jnp.int32(0)
    for j in range(half):
        local = sources[own + j] - own
        away = (local < 0) | (local >= half)
        pick[j] = jnp.where(away, half + jnp.minimum(rank, crossing - 1), local)
        rank = rank + jnp.where(away, 1, 0)
    rank = jnp.int32(0)
    found = [jnp.int32(0)] * crossing
    for j in range(half):
        local = sources[other + j] - own
        here = (local >= 0) & (local < half)
        for i in range(min(j + 1, crossing)):
            found[i] = jnp.where(here & (rank == i), local, found[i])
        rank = rank + jnp.where(here, 1, 0)
    for i in range(crossing):
        cross[i] = found[i]


def selection(matrix, table, rows):
    shape = (rows, matrix.shape[1])
    row = lax.broadcasted_iota(jnp.int32, shape, 0)
    column = lax.broadcasted_iota(jnp.int32, shape, 1)
    for j in range(table.shape[0]):
        chosen = column == table[j] * rows + row
        matrix[j * rows : (j + 1) * rows, :] = jnp.where(chosen, 1.0, 0.0).astype(jnp.bfloat16)


def select(matrix, blocks):
    slots, rows, width = blocks.shape
    flat = blocks.astype(jnp.float32).reshape(slots * rows, width).astype(jnp.bfloat16)
    value = jnp.dot(matrix[...], flat, preferred_element_type=jnp.float32)
    return value.reshape(matrix.shape[0] // rows, rows, width).astype(jnp.bfloat16)


def pipeline(count, stages):
    @pl.loop(0, count + max(lag for _, lag in stages))
    def _(t):
        for stage, lag in stages:
            @pl.when((t >= lag) & (t < count + lag))
            def _():
                stage(t - lag)


class Layout:
    def __init__(self, g, me, n, width):
        self.half, self.relays = n // 2, n // 4
        self.count, self.w = chunking(width, self.relays)
        self.wide = self.relays * self.w
        self.pairs = max(1, self.relays // PAIR)
        self.group = self.relays // self.pairs
        self.g, self.me = g, me
        self.h, self.slot = me // self.half, lax.rem(me, self.half)
        self.base = self.h * self.half
        self.r = lax.rem(me, self.relays)
        self.is_relay = me // self.relays == 1 + self.h
        self.outer = self.base + self.h * self.relays
        self.outer_slot = self.h * self.relays
        self.first = (1 + self.h) * self.relays
        self.partner = me + self.relays - 2 * self.relays * self.h
        self.line, self.lane = self.r // self.group, lax.rem(self.r, self.group)

    def piece(self, c, rr, size=1):
        return pl.ds(pl.multiple_of(c * self.wide + rr * self.w, self.w), size * self.w)

    def chunk(self, c):
        return pl.ds(pl.multiple_of(c * self.wide, self.wide), self.wide)


class Route:
    def __init__(self, lay, crossing, early, take, put, load, store, pick, cross, bufs, sems):
        self.lay, self.crossing, self.take, self.put = lay, crossing, take, put
        self.load, self.store, self.pick, self.cross = load, store, pick, cross
        self.side, self.pool, self.over, self.deal = bufs
        self.s_direct, self.s_early, self.s_side, self.s_onward, self.s_across, self.s_give = sems[:6]
        self.r_direct, self.r_side, self.r_across, self.r_give = sems[6:]
        self.early, self.late = early
        self.few = self.early + self.late

    def several(self, ref, send, recv):
        return remote(ref, ref, send, recv, (self.lay.g, self.lay.partner))

    def direct(self, c, rr, send):
        l = self.lay
        return remote(self.take(c, rr, 1), self.pool.at[c, l.slot], send, self.r_direct.at[c], (l.g, l.first + rr))

    def sideways(self, c, line):
        l = self.lay
        return remote(
            self.take(c, line * l.group, l.group), self.side.at[c, l.line], self.s_side, self.r_side.at[c],
            (l.g, l.outer + line * l.group + l.lane),
        )

    def onward(self, c, line, q):
        l = self.lay
        return remote(
            self.side.at[c, line, :, pl.ds(q * l.w, l.w)], self.pool.at[c, l.outer_slot + line * l.group + l.lane],
            self.s_onward, self.r_direct.at[c], (l.g, l.first + l.line * l.group + q),
        )

    def across(self, c):
        l = self.lay
        return remote(
            self.over.at[c], self.pool.at[c, pl.ds(l.half, self.crossing)], self.s_across, self.r_across.at[c], (l.g, l.partner)
        )

    def give(self, c, j):
        l = self.lay
        return remote(self.deal.at[c, j], self.put(c, l.r, 1), self.s_give, self.r_give.at[c], (l.g, l.base + j))

    def lines(self, stage):
        l = self.lay
        for line in range(l.pairs):
            pl.when(jnp.logical_not(l.is_relay) & (line != l.line))(functools.partial(stage, line))

    def through(self, c):
        return (c >= self.early) & (c < self.lay.count - self.late)

    def start_far(self, c):
        def stage(line):
            @pl.when(self.through(c))
            def _():
                self.sideways(c, line).start()

            @pl.when(jnp.logical_not(self.through(c)))
            def _():
                for q in range(self.lay.group):
                    self.direct(c, line * self.lay.group + q, self.s_early).start()

        self.lines(stage)

    def start_near(self, c):
        l = self.lay
        for rr in range(l.relays):
            near = jnp.where(l.is_relay, rr != l.r, rr // l.group == l.line)
            pl.when(near)(lambda rr=rr: self.direct(c, rr, self.s_direct).start())

    def forward(self, c):
        l = self.lay

        def stage(line):
            for q in range(l.group):
                self.onward(c, line, q).start()

        if l.pairs > 1:
            @pl.when(jnp.logical_not(l.is_relay) & self.through(c))
            def _():
                self.several(self.side.at[c, pl.ds(0, l.pairs - 1)], self.s_side, self.r_side.at[c]).wait_recv()
                self.lines(stage)

    def collect(self, c):
        l = self.lay

        @pl.when(l.is_relay)
        def _():
            self.pool[c, l.slot] = self.load(c, l.r)
            self.several(self.pool.at[c, pl.ds(0, l.half - 1)], self.s_direct, self.r_direct.at[c]).wait_recv()
            self.over[c] = select(self.cross, self.pool[c, : l.half])
            self.across(c).start()

    def hand(self, c):
        l = self.lay

        @pl.when(l.is_relay)
        def _():
            self.across(c).wait_recv()
            self.deal[c] = select(self.pick, self.pool[c])
            for k in range(1, l.half):
                self.give(c, lax.rem(l.slot + k, l.half)).start()
            self.store(c, l.r, self.deal[c, l.slot])

    def arrive(self, c):
        l = self.lay

        @pl.when(l.is_relay)
        def _():
            self.several(self.put(c, 0, l.relays - 1), self.s_give, self.r_give.at[c]).wait_recv()

        @pl.when(jnp.logical_not(l.is_relay))
        def _():
            self.several(self.put(c, 0, l.relays), self.s_give, self.r_give.at[c]).wait_recv()

    def drain(self):
        l = self.lay

        @pl.when(l.is_relay)
        def _():
            self.several(self.pool.at[:, pl.ds(0, l.relays - 1)], self.s_direct, self.r_direct.at[0]).wait_send()
            self.several(self.over, self.s_across, self.r_across.at[0]).wait_send()
            self.several(self.deal.at[:, pl.ds(0, l.half - 1)], self.s_give, self.r_give.at[0]).wait_send()

        @pl.when(jnp.logical_not(l.is_relay))
        def _():
            self.several(self.pool.at[:, pl.ds(0, l.group)], self.s_direct, self.r_direct.at[0]).wait_send()
            if l.pairs > 1:
                sent = self.side.at[pl.ds(0, l.count - self.few), pl.ds(0, l.pairs - 1)]
                if self.few:
                    first = self.pool.at[pl.ds(0, self.few), pl.ds(0, l.relays - l.group)]
                    self.several(first, self.s_early, self.r_side.at[0]).wait_send()
                self.several(sent, self.s_side, self.r_side.at[0]).wait_send()
                self.several(sent, self.s_onward, self.r_side.at[0]).wait_send()


def fused_kernel(d, n, crossing, old, new, routed_hbm, ids, probe, gain, gate_hbm, up_hbm, down_hbm, out, totals,
                 wg, wu, wd, routed, normed, x, gate_sum, up_sum, hidden, partial, arrived, summed,
                 stats, st_in, st_mid, st_dp, source, holder, order, crossed, pick, cross, pick2, cross2, sl, sw, sd,
                 sy, ry, ss, rs, ssy, rsy, sz, rz, *rest):
    g, me = lax.axis_index("dp"), lax.axis_index("expert")
    rows, width = normed.shape
    lay = Layout(g, me, n, width)
    count, wide, w = lay.count, lay.wide, lay.w
    chunk, piece = lay.chunk, lay.piece
    tall = d * rows
    down_parts = 8
    down_step = wd.shape[0] // down_parts

    load_routed = pltpu.make_async_copy(routed_hbm, routed, sl)
    load_routed.start()
    greet(g, me, d, n)
    weights, downs = [], []
    for c in range(count):
        part = pl.ds(c * wide, wide)
        weights.append(pltpu.make_async_copy(gate_hbm.at[part, :], wg.at[part, :], sw.at[c]))
        weights.append(pltpu.make_async_copy(up_hbm.at[part, :], wu.at[part, :], sw.at[c]))
    for p in range(down_parts):
        part = pl.ds(p * down_step, down_step)
        downs.append(pltpu.make_async_copy(down_hbm.at[part, :], wd.at[part, :], sd))
    load_routed.wait()
    for load in weights + downs:
        load.start()
    mean_square = prepare(routed, probe, gain, normed)
    meet(d, n)

    def put_x(c, rr, value):
        x[g, :, piece(c, rr)] = value

    def put_out(c, rr, value):
        out[:, piece(c, rr)] = value

    there = Route(
        lay, crossing, direct_chunks(count, FIRST),
        lambda c, rr, size: normed.at[:, piece(c, rr, size)], lambda c, rr, size: x.at[g, :, piece(c, rr, size)],
        lambda c, rr: normed[:, piece(c, rr)], put_x, pick, cross, rest[0:4], rest[8:18],
    )
    summed_piece = lambda rr, size: pl.ds(pl.multiple_of(rr * w, w), size * w)
    home = Route(
        lay, crossing, direct_chunks(count, SECOND),
        lambda c, rr, size: summed.at[c, :, summed_piece(rr, size)], lambda c, rr, size: out.at[:, piece(c, rr, size)],
        lambda c, rr: summed[c, :, summed_piece(rr, 1)], put_out, pick2, cross2, rest[4:8], rest[18:28],
    )

    def peers(ref, send, recv):
        return remote(ref, ref, send, recv, (lax.rem(g + 1, d), me))

    def along(c, q):
        here = x.at[g, :, chunk(c)]
        return remote(here, here, sy, ry.at[c], (lax.rem(g + q, d), me))

    def stat(k):
        return remote(stats, st_in.at[me], ss, rs, (g, lax.rem(me + k, n)))

    def stat_all():
        part = st_in.at[pl.ds(0, n - 1)]
        return remote(part, part, ss, rs, (g, lay.partner))

    def stat_dp(q):
        return remote(st_mid, st_dp.at[g], ssy, rsy, (lax.rem(g + q, d), me))

    ahead = min(AHEAD, count)
    pl.loop(0, count)(there.start_far)
    pl.loop(0, ahead)(there.start_near)
    pl.when(lay.is_relay)(lambda: pl.loop(ahead, count)(there.start_near))

    @pl.when(jnp.logical_not(lay.is_relay))
    def _():
        @pl.loop(0, count)
        def _(c):
            there.forward(c)
            pl.when(c + ahead < count)(lambda: there.start_near(c + ahead))

    inverse(old, new, source, n)
    inverse(new, old, holder, n)
    for places, picks, crosses in ((source, pick, cross), (holder, pick2, cross2)):
        plan(places, lay.h, lay.half, crossing, order, crossed)
        selection(picks, order, rows)
        selection(crosses, crossed, rows)
    statistics(ids, mean_square, stats)
    for k in range(1, n):
        stat(k).start()
    st_in[me] = stats[...]
    gate_sum[...] = jnp.zeros_like(gate_sum)
    up_sum[...] = jnp.zeros_like(up_sum)

    def take(c):
        there.arrive(c)
        for q in range(1, d):
            along(c, q).start()

    def absorb(c):
        if d > 1:
            peers(x.at[pl.ds(0, d - 1), :, chunk(c)], sy, ry.at[c]).wait_recv()
        part = x[:, :, chunk(c)].astype(jnp.float32).reshape(tall, wide).astype(jnp.bfloat16)
        both = pl.ds(0, 2 * wide)
        pltpu.make_async_copy(gate_hbm.at[both, :], wg.at[both, :], sw.at[c]).wait()
        for ref, total in ((wg, gate_sum), (wu, up_sum)):
            total[...] += jnp.dot(part, ref[chunk(c), :], preferred_element_type=jnp.float32)

    lags = LAGS[count] if count in LAGS else LAGS[7]
    pipeline(count, [(there.collect, 0), (there.hand, lags[0]), (take, lags[1]), (absorb, lags[2])])

    gate = gate_sum[...]
    hidden[...] = (gate / (1.0 + jnp.exp(-gate)) * up_sum[...]).astype(jnp.bfloat16)
    pltpu.make_async_copy(down_hbm, wd, sd).wait()

    def home_copy(c, q):
        return remote(partial.at[c, lax.rem(g + q, d)], arrived.at[c, q - 1], sz, rz.at[c], (lax.rem(g + q, d), me))

    def make(c):
        value = jnp.dot(hidden[...], wd[:, chunk(c)], preferred_element_type=jnp.float32)
        partial[c] = value.reshape(d, rows, wide).astype(jnp.bfloat16)
        for q in range(1, d):
            home_copy(c, q).start()

    def add(c):
        total = partial[c, g].astype(jnp.float32)
        if d > 1:
            peers(arrived.at[c], sz, rz.at[c]).wait_recv()
        for q in range(1, d):
            total = total + arrived[c, q - 1].astype(jnp.float32)
        summed[c] = total.astype(jnp.bfloat16)
        home.start_far(c)
        home.start_near(c)

    stat_all().wait_recv()
    mid = st_in[0]
    for s in range(1, n):
        mid = mid + st_in[s]
    st_mid[...] = mid
    st_dp[g] = mid
    for q in range(1, d):
        stat_dp(q).start()

    pipeline(count, [
        (make, 0), (add, lags[3]), (home.forward, lags[4]), (home.collect, lags[5]), (home.hand, lags[6]),
    ])

    stat_all().wait_send()
    if d > 1:
        peers(st_dp.at[pl.ds(0, d - 1)], ssy, rsy).wait()
        peers(x.at[pl.ds(0, d - 1)], sy, ry.at[0]).wait_send()
        peers(arrived, sz, rz.at[0]).wait_send()
    total = st_dp[0]
    for f in range(1, d):
        total = total + st_dp[f]
    totals[...] = total

    there.drain()
    home.drain()
    pl.loop(0, count)(home.arrive)


def fused(crossing, collective, d, n, experts, old, new, routed, ids, probe, gain, gate, up, down):
    tokens, width = routed.shape
    rows = probe.shape[1]
    units = gate.shape[1]
    lay = Layout(0, 0, n, width)
    count, w, half, relays, pairs, group = lay.count, lay.w, lay.half, lay.relays, lay.pairs, lay.group
    full = lay.wide
    dma = pltpu.SemaphoreType.DMA
    block = lambda *shape: pltpu.VMEM(shape, jnp.bfloat16)
    wide = lambda *shape: pltpu.VMEM(shape, jnp.float32)
    numbers = lambda size: pltpu.SMEM((size,), jnp.int32)
    matrices = [block(half * rows, (half + crossing) * rows), block(crossing * rows, half * rows)]
    bufs = [
        block(count, pairs, rows, group * w), block(count, half + crossing, rows, w),
        block(count, crossing, rows, w), block(count, half, rows, w),
    ]
    sems = [dma, dma, dma, dma, dma, dma, dma((count,)), dma((count,)), dma((count,)), dma((count,))]
    return pl.pallas_call(
        functools.partial(fused_kernel, d, n, crossing),
        out_shape=(
            jax.ShapeDtypeStruct((rows, width), jnp.bfloat16),
            jax.ShapeDtypeStruct((2, experts), jnp.float32),
        ),
        in_specs=[SMEM, SMEM, HBM, VMEM, VMEM, VMEM, HBM, HBM, HBM],
        out_specs=(VMEM, VMEM),
        scratch_shapes=[
            block(width, units), block(width, units), block(units, width),
            block(tokens, width), block(rows, width), block(d, rows, width),
            wide(d * rows, units), wide(d * rows, units), block(d * rows, units),
            block(count, d, rows, full), block(count, max(1, d - 1), rows, full), block(count, rows, full),
            wide(2, experts), wide(n, 2, experts), wide(2, experts), wide(d, 2, experts),
            numbers(n), numbers(n), numbers(half), numbers(crossing), *matrices, *matrices,
            dma, dma((count,)), dma,
            dma, dma((count,)), dma, dma, dma, dma, dma, dma((count,)),
            *bufs, *bufs, *sems, *sems,
        ],
        compiler_params=pltpu.CompilerParams(
            collective_id=collective, has_side_effects=True, vmem_limit_bytes=125 << 19
        ),
    )(old, new, routed, ids, probe, gain, gate, up, down)


def on_device(
    routed,
    expert_ids,
    norm_gain,
    gate_weight,
    up_weight,
    down_weight,
    old_place,
    new_place,
    probe_ids,
):
    n, d = lax.axis_size("expert"), lax.axis_size("dp")
    experts = EXP_DEV * n
    tokens = routed.shape[0] * d * n
    half = n // 2
    widths = (half // 2, half * 5 // 8, half)
    index = jnp.arange(n, dtype=jnp.int32)
    apart = (index[:, None] < half) & (index[None, :] >= half)
    crossings = jnp.sum(((old_place[:, None] == new_place[None, :]) & apart).astype(jnp.int32))
    branch = (crossings > widths[0]).astype(jnp.int32) + (crossings > widths[1]).astype(jnp.int32)
    kernels = [functools.partial(fused, widths[i], i, d, n, experts) for i in range(3)]
    probe_out, totals = lax.switch(
        branch, kernels,
        old_place, new_place, routed, expert_ids.T, probe_ids.reshape(1, -1), norm_gain,
        gate_weight[0], up_weight[0], down_weight[0],
    )
    owned = lax.dynamic_slice_in_dim(totals, lax.axis_index("expert") * EXP_DEV, EXP_DEV, 1)
    expert_load = owned[0] * experts / (tokens * expert_ids.shape[1])
    expert_energy = owned[1] / owned[0]
    return (expert_load, expert_energy, probe_out)


def solution(mesh):
    in_specs = (
        P(("dp", "expert"), None),
        P(("dp", "expert"), None),
        P(),
        P("expert", None, "dp"),
        P("expert", None, "dp"),
        P("expert", "dp", None),
        P(),
        P(),
        P(("dp", "expert")),
    )
    out_specs = (P("expert"), P("expert"), P(("dp", "expert"), None))
    return jax.shard_map(
        on_device, mesh=mesh, in_specs=in_specs, out_specs=out_specs, check_vma=False
    )
```
